32 devices in a mesh: pair: 4 (over y, x), aux: 8 (over z, core).
Axes of the slice: x: 2, y: 2, z: 4, core: 2. Of those that a mesh axis runs over, the one named last changes fastest.
Arguments:
- same_panels: bfloat16 [32, 2, 112, 59904], P('aux', None, None, 'pair'), may hold values from -1 to 1
- opposite_panels: bfloat16 [32, 2, 112, 59904], P('aux', None, None, 'pair'), may hold values from -1 to 1
- same_amplitudes: bfloat16 [32, 112, 112], replicated, may hold values from -2 to 2
- opposite_amplitudes: bfloat16 [32, 112, 112], replicated, may hold values from -2 to 2
- same_energies: float32 [32, 2, 112], replicated, may hold values from 0.5 to 3
- opposite_energies: float32 [32, 2, 112], replicated, may hold values from 0.5 to 3
- same_ranks: int32 [32], replicated, may hold values from 48 to 112
- opposite_ranks: int32 [32], replicated, may hold values from 48 to 112
Outputs:
- same_residual: float32 [32, 112, 112], P('pair', 'aux')
- opposite_residual: float32 [32, 112, 112], P('pair', 'aux')
The draws below stay inside these ranges and needn't reach their ends.
Inputs may be any that keep to these rules, and one draw needn't show every extreme that they name: `same_ranks`: slots at or beyond a pair's rank are padding. `opposite_ranks`: slots at or beyond a pair's rank are padding.
All inputs are finite; a program needn't handle non-finite values.
Results may differ from the reference program's by a relative error of at most 0.0013.
Values may be sent and summed in bfloat16 or wider, within the bound.
A program may use at most 128 MiB of HBM per device.

```python
import math
import jax
import jax.numpy as jnp
from jax import lax

R = 112
NAUX = 59904
PAIRS = 32


def with_ends(entries, key, least, top_value):
    dims = entries.shape
    index_at = [jax.random.randint(jax.random.fold_in(key, axis), (), 0, dims[axis]) for axis in range(len(dims))]
    entries = entries.at[tuple(index_at)].set(least)
    longest = dims.index(max(dims))
    index_at[longest] = (index_at[longest] + 1) % dims[longest]
    return entries.at[tuple(index_at)].set(top_value)


def steps_of(own_key, extent, shards, smallest, largest):
    def one(position, parts):
        heights = jax.random.uniform(jax.random.fold_in(jax.random.fold_in(own_key, 6), position), (parts,), jnp.float32, smallest / len(shards), largest / len(shards))
        return jnp.repeat(jnp.exp(heights), extent[position] // parts).reshape((-1,) + (1,) * (len(extent) - position - 1))

    level = one(*shards[0])
    for cut in shards[1:]:
        level = level * one(*cut)
    return level


def bell_draw(stream_key, shape, deviation, limit, pieces=(), kind=jnp.bfloat16):
    factor_of = steps_of(stream_key, shape, pieces, -0.22, 0.18) if pieces else 1.0
    values = jax.random.normal(stream_key, shape, jnp.float32) * deviation * factor_of
    return jnp.minimum(jnp.maximum(values, -limit), limit).astype(kind)


def setup_inputs(seed: int = 0) -> dict:
    arg_keys = jax.random.split(jax.random.key(seed), 9)
    same_panels = bell_draw(arg_keys[0], (PAIRS, 2, R, NAUX), (NAUX ** -0.25), 1.0, ((0, 8), (3, 4)))
    opposite_panels = bell_draw(arg_keys[1], (PAIRS, 2, R, NAUX), (NAUX ** -0.25), 1.0, ((0, 8), (3, 4)))
    same_amplitudes = bell_draw(arg_keys[2], (PAIRS, R, R), 0.15, 2.0)
    opposite_amplitudes = bell_draw(arg_keys[3], (PAIRS, R, R), 0.15, 2.0)
    same_energies = jnp.clip(jnp.exp(jax.random.uniform(arg_keys[4], (PAIRS, 2, R), jnp.float32, math.log(0.5), math.log(3.0))), 0.5, 3.0)
    opposite_energies = jnp.clip(jnp.exp(jax.random.uniform(arg_keys[5], (PAIRS, 2, R), jnp.float32, math.log(0.5), math.log(3.0))), 0.5, 3.0)
    same_ranks = with_ends(jax.random.randint(arg_keys[6], (PAIRS,), R * 3 // 7, R + 1), jax.random.fold_in(arg_keys[6], 1), R * 3 // 7, R).astype(jnp.int32)
    opposite_ranks = with_ends(jax.random.randint(arg_keys[7], (PAIRS,), R * 3 // 7, R + 1), jax.random.fold_in(arg_keys[7], 1), R * 3 // 7, R).astype(jnp.int32)
    return dict(same_panels=same_panels, opposite_panels=opposite_panels, same_amplitudes=same_amplitudes, opposite_amplitudes=opposite_amplitudes, same_energies=same_energies, opposite_energies=opposite_energies, same_ranks=same_ranks, opposite_ranks=opposite_ranks)


def slot_mask(ranks):
    slots = jnp.arange(R, dtype=jnp.int32)
    return (slots[None, :] < ranks[:, None]).astype(jnp.float32)


def masked_amplitudes(amplitudes, keep):
    outer = keep[:, :, None] * keep[:, None, :]
    return (amplitudes.astype(jnp.float32) * outer).astype(jnp.bfloat16)


def dressing_rows(panels, masked):
    def one_pair(items):
        panel, amplitude = items
        mixed = jnp.dot(amplitude, panel[1], preferred_element_type=jnp.float32)
        return jnp.sum(panel[0].astype(jnp.float32) * mixed, axis=0)
    return lax.map(one_pair, (panels, masked))


def residual_rows(panels, masked, energies, keep, coupling):
    def one_pair(items):
        panel, amplitude, energy, mask_row = items
        exchange = jnp.dot(panel[0], panel[1].T, preferred_element_type=jnp.float32)
        scaled = (panel[0].astype(jnp.float32) * coupling[None, :]).astype(jnp.bfloat16)
        coulomb = jnp.dot(scaled, panel[1].T, preferred_element_type=jnp.float32)
        diagonal = (energy[0][:, None] + energy[1][None, :]) * amplitude.astype(jnp.float32)
        return (exchange + coulomb + diagonal) * (mask_row[:, None] * mask_row[None, :])
    return lax.map(one_pair, (panels, masked, energies, keep))


def reference(same_panels, opposite_panels, same_amplitudes, opposite_amplitudes, same_energies, opposite_energies, same_ranks, opposite_ranks):
    same_keep = slot_mask(same_ranks)
    opposite_keep = slot_mask(opposite_ranks)
    same_masked = masked_amplitudes(same_amplitudes, same_keep)
    opposite_masked = masked_amplitudes(opposite_amplitudes, opposite_keep)
    coupling = jnp.sum(dressing_rows(same_panels, same_masked), axis=0) + jnp.sum(dressing_rows(opposite_panels, opposite_masked), axis=0)
    same_residual = residual_rows(same_panels, same_masked, same_energies, same_keep, coupling)
    opposite_residual = residual_rows(opposite_panels, opposite_masked, opposite_energies, opposite_keep, coupling)
    return same_residual, opposite_residual
```

```python
import functools

import jax
import jax.numpy as jnp
from jax import lax
from jax.experimental import pallas as pl
from jax.experimental.pallas import tpu as pltpu
from jax.sharding import PartitionSpec as P

LANES = 128
GROUP = 2
LAG = 2
UNROLL = 4


def rows_dot(first, second):
    return lax.dot_general(
        first, second, (((1,), (1,)), ((), ())), preferred_element_type=jnp.float32
    )


def kernel(
    plan,
    same_ref,
    opposite_ref,
    same_amplitudes,
    opposite_amplitudes,
    same_energies,
    opposite_energies,
    same_ranks,
    opposite_ranks,
    same_out,
    opposite_out,
    panel,
    total,
    partial,
    flat,
    share,
    arrived,
    amplitude,
    energy,
    staged,
    out_a,
    in_a,
    out_b,
    in_b,
    rank,
    load_sem,
    small_sem,
    share_send,
    share_recv,
    a_send,
    a_recv,
    b_send,
    b_recv,
    store_sem,
):
    pairs, auxes, count, slots, steps, width = plan
    sources = (same_ref, opposite_ref)
    outs = (same_out, opposite_out)
    fold = auxes // pairs
    rows = slots // auxes
    block = 2 * count
    groups = block // GROUP
    me_pair = lax.axis_index("pair")
    me_aux = lax.axis_index("aux")

    mine = pl.ds(me_aux * count, count)
    small = []
    for spin, (amps, gaps, ranks) in enumerate(
        (
            (same_amplitudes, same_energies, same_ranks),
            (opposite_amplitudes, opposite_energies, opposite_ranks),
        )
    ):
        here = pl.ds(spin * count, count)
        small.append(
            pltpu.make_async_copy(amps.at[mine], amplitude.at[here], small_sem.at[0, spin])
        )
        small.append(pltpu.make_async_copy(gaps.at[mine], energy.at[here], small_sem.at[1, spin]))
        small.append(pltpu.make_async_copy(ranks, rank.at[spin], small_sem.at[2, spin]))
    for copy in small:
        copy.start()

    def lanes(step):
        return pl.ds(pl.multiple_of(step * width, LANES), width)

    def load(step, spin, pair):
        at = lanes(step)
        return pltpu.make_async_copy(
            sources[spin].at[pair, :, :, at],
            panel.at[spin * count + pair, :, :, at],
            load_sem.at[step, spin * count + pair],
        )

    @pl.loop(0, steps)
    def _(step):
        for spin in range(2):

            @pl.loop(0, count)
            def _(pair):
                load(step, spin, pair).start()

    barrier = pltpu.get_barrier_semaphore()
    devices = pairs * auxes
    me = me_pair * auxes + me_aux

    @pl.loop(1, devices)
    def _(ahead):
        other = lax.rem(me + ahead, devices)
        pl.semaphore_signal(
            barrier,
            inc=1,
            device_id=(lax.div(other, auxes), lax.rem(other, auxes)),
            device_id_type=pl.DeviceIdType.MESH,
        )

    for copy in small:
        copy.wait()
    row_at = lax.broadcasted_iota(jnp.int32, (slots, slots), 0)
    column_at = lax.broadcasted_iota(jnp.int32, (slots, slots), 1)

    def kept(place):
        bound = rank[place // count, me_aux * count + place % count]
        return jnp.logical_and(row_at < bound, column_at < bound)

    owns_diagonal = (me_pair == 0).astype(jnp.float32)
    for place in range(block):
        full = amplitude[place].astype(jnp.float32)
        masked = jnp.where(kept(place), full, 0.0)
        first_gap = jnp.sum(
            jnp.where(row_at == column_at, energy[place, 0:1, :], 0.0), axis=1, keepdims=True
        )
        gap = first_gap + energy[place, 1:2, :]
        total[place] = gap * masked * owns_diagonal
        amplitude[place] = masked.astype(jnp.bfloat16)

    def dress(place, step):
        at = lanes(step)
        mixed = jnp.dot(
            amplitude[place], panel[place, 1, :, at], preferred_element_type=jnp.float32
        )
        product = panel[place, 0, :, at].astype(jnp.float32) * mixed
        return jnp.sum(product.reshape(slots // 8, 8, width), axis=0)

    def both_terms(place, step):
        at = lanes(step)
        left = panel[place, 0, :, at]
        scaled = (left.astype(jnp.float32) * flat[:, at]).astype(jnp.bfloat16)
        value = rows_dot(jnp.concatenate([left, scaled], axis=0), panel[place, 1, :, at])
        return value[:slots] + value[slots:]

    def peer_share(step, ahead):
        return pltpu.make_async_remote_copy(
            src_ref=share.at[step],
            dst_ref=arrived.at[step, ahead],
            send_sem=share_send.at[step, ahead],
            recv_sem=share_recv.at[step, ahead],
            device_id=(me_pair, lax.rem(me_aux + ahead, auxes)),
            device_id_type=pl.DeviceIdType.MESH,
        )

    def send_share(step):
        share[step] = jnp.sum(partial[...], axis=0, keepdims=True)
        for ahead in range(1, auxes):
            peer_share(step, ahead).start()

    def sum_shares(step):
        value = share[step]
        for ahead in range(1, auxes):
            peer_share(step, ahead).wait_recv()
            value = value + arrived[step, ahead]
        flat[:, lanes(step)] = value

    def sweep(step, with_terms):
        partial[...] = jnp.zeros_like(partial)

        @pl.loop(0, block // UNROLL)
        def _(turn):
            first = turn * UNROLL
            for spin in range(2):

                @pl.when(lax.div(first, count) == spin)
                def _():
                    for inner in range(UNROLL):
                        load(step, spin, first + inner - spin * count).wait()

            value = partial[...]
            for inner in range(UNROLL):
                value = value + dress(first + inner, step)
                if with_terms:
                    total[first + inner] += both_terms(first + inner, step - LAG)
            partial[...] = value

    sweep(0, False)
    pl.semaphore_wait(barrier, devices - 1)
    send_share(0)

    @pl.loop(1, LAG)
    def _(step):
        sweep(step, False)
        send_share(step)

    @pl.loop(LAG, steps)
    def _(step):
        sum_shares(step - LAG)
        sweep(step, True)
        send_share(step)

    @pl.loop(steps - LAG, steps - 1)
    def _(step):
        sum_shares(step)

        @pl.loop(0, block // UNROLL)
        def _(turn):
            for inner in range(UNROLL):
                total[turn * UNROLL + inner] += both_terms(turn * UNROLL + inner, step)

    sum_shares(steps - 1)

    def send_a(group, ahead):
        other = lax.rem(me_pair + ahead, pairs)
        return pltpu.make_async_remote_copy(
            src_ref=out_a.at[other, group],
            dst_ref=in_a.at[ahead, group],
            send_sem=a_send.at[ahead, group],
            recv_sem=a_recv.at[ahead, group],
            device_id=(other, me_aux),
            device_id_type=pl.DeviceIdType.MESH,
        )

    owner = lax.div(me_aux, fold)
    slot = lax.rem(me_aux, fold)

    def send_b(group, part):
        return pltpu.make_async_remote_copy(
            src_ref=out_b.at[group, part],
            dst_ref=in_b.at[slot, group],
            send_sem=b_send.at[part, group],
            recv_sem=b_recv.at[slot, group],
            device_id=(owner, me_pair * fold + part),
            device_id_type=pl.DeviceIdType.MESH,
        )

    def stays(part):
        return jnp.logical_and(owner == me_pair, me_pair * fold + part == me_aux)

    def arrival_b(group, part):
        return pltpu.make_async_remote_copy(
            src_ref=out_b.at[group, part],
            dst_ref=in_b.at[part, group],
            send_sem=b_send.at[part, group],
            recv_sem=b_recv.at[part, group],
            device_id=(owner, me_pair * fold + part),
            device_id_type=pl.DeviceIdType.MESH,
        )

    def forward(group):
        held = out_a[me_pair, group]
        for ahead in range(1, pairs):
            send_a(group, ahead).wait_recv()
            held = held + in_a[ahead, group]
        out_b[group] = held
        for part in range(fold):

            @pl.when(jnp.logical_not(stays(part)))
            def _():
                send_b(group, part).start()

            @pl.when(stays(part))
            def _():
                in_b[part, group] = out_b[group, part]

    for group in range(groups):
        for inner in range(GROUP):
            place = group * GROUP + inner
            value = total[place] + both_terms(place, steps - 1)
            value = jnp.where(kept(place), value, 0.0)
            for quarter in range(pairs):
                for part in range(fold):
                    first = (quarter * fold + part) * rows
                    out_a[quarter, group, part, inner, 0:rows, 0:slots] = value[
                        first : first + rows, :
                    ]
        for ahead in range(1, pairs):
            send_a(group, ahead).start()
        if group > 0:
            forward(group - 1)
    forward(groups - 1)

    def store(spin):
        return pltpu.make_async_copy(staged.at[spin], outs[spin], store_sem.at[spin])

    for group in range(groups):
        for part in range(fold):

            @pl.when(jnp.logical_not(stays(part)))
            def _():
                arrival_b(group, part).wait_recv()

            for inner in range(GROUP):
                place = group * GROUP + inner
                staged[place // count, part * count + place % count] = in_b[
                    part, group, inner, 0:rows, 0:slots
                ]
        if (group + 1) * GROUP % count == 0:
            store((group + 1) * GROUP // count - 1).start()

    @pl.loop(0, steps)
    def _(step):
        for ahead in range(1, auxes):
            peer_share(step, ahead).wait_send()

    for group in range(groups):
        for ahead in range(1, pairs):
            send_a(group, ahead).wait_send()
        for part in range(fold):

            @pl.when(jnp.logical_not(stays(part)))
            def _():
                send_b(group, part).wait_send()

    for spin in range(2):
        store(spin).wait()


def residuals(
    same_panels,
    opposite_panels,
    same_amplitudes,
    opposite_amplitudes,
    same_energies,
    opposite_energies,
    same_ranks,
    opposite_ranks,
    pairs,
    auxes,
):
    if same_panels.shape[3] % LANES:
        extra = ((0, 0), (0, 0), (0, 0), (0, -same_panels.shape[3] % (8 * LANES)))
        same_panels = jnp.pad(same_panels, extra)
        opposite_panels = jnp.pad(opposite_panels, extra)
    count, _, slots, length = same_panels.shape
    tiles = length // LANES
    steps = next(parts for parts in range(min(8, tiles), tiles + 1) if tiles % parts == 0)
    width = length // steps
    fold = auxes // pairs
    rows = slots // auxes
    tall = -(-rows // 8) * 8
    wide = -(-slots // LANES) * LANES
    block = 2 * count
    groups = block // GROUP
    plan = (pairs, auxes, count, slots, steps, width)
    piece = (GROUP, tall, wide)
    shape = jax.ShapeDtypeStruct((count * fold, rows, slots), jnp.float32)
    anywhere = pl.BlockSpec(memory_space=pl.ANY)
    dma = pltpu.SemaphoreType.DMA
    return pl.pallas_call(
        functools.partial(kernel, plan),
        out_shape=(shape, shape),
        in_specs=[anywhere] * 8,
        out_specs=(anywhere, anywhere),
        scratch_shapes=[
            pltpu.VMEM((block, 2, slots, length), jnp.bfloat16),
            pltpu.VMEM((block, slots, slots), jnp.float32),
            pltpu.VMEM((8, width), jnp.float32),
            pltpu.VMEM((1, length), jnp.float32),
            pltpu.VMEM((steps, 1, width), jnp.float32),
            pltpu.VMEM((steps, auxes, 1, width), jnp.float32),
            pltpu.VMEM((block, slots, slots), jnp.bfloat16),
            pltpu.VMEM((block, 2, slots), jnp.float32),
            pltpu.VMEM((2, count * fold, rows, slots), jnp.float32),
            pltpu.VMEM((pairs, groups, fold) + piece, jnp.float32),
            pltpu.VMEM((pairs, groups, fold) + piece, jnp.float32),
            pltpu.VMEM((groups, fold) + piece, jnp.float32),
            pltpu.VMEM((fold, groups) + piece, jnp.float32),
            pltpu.SMEM((2, same_ranks.shape[0]), jnp.int32),
            dma((steps, block)),
            dma((3, 2)),
            dma((steps, auxes)),
            dma((steps, auxes)),
            dma((pairs, groups)),
            dma((pairs, groups)),
            dma((fold, groups)),
            dma((fold, groups)),
            dma((2,)),
        ],
        compiler_params=pltpu.CompilerParams(
            collective_id=0, has_side_effects=True, vmem_limit_bytes=67043328
        ),
        name="residuals",
    )(
        same_panels,
        opposite_panels,
        same_amplitudes,
        opposite_amplitudes,
        same_energies,
        opposite_energies,
        same_ranks,
        opposite_ranks,
    )


def solution(mesh):
    placed = (P("aux", None, None, "pair"),) * 2 + (P(),) * 6
    return jax.shard_map(
        functools.partial(residuals, pairs=mesh.shape["pair"], auxes=mesh.shape["aux"]),
        mesh=mesh,
        in_specs=placed,
        out_specs=(P("pair", "aux", None), P("pair", "aux", None)),
        check_vma=False,
    )
```
